32 devices in a mesh: section: 2 (over core), dp: 4 (over z), tensor: 4 (over y, x).
Axes of the slice: x: 2, y: 2, z: 4, core: 2. Of those that a mesh axis runs over, the one named last changes fastest.
Arguments:
- inputs: bfloat16 [2, 512, 4096], P(None, 'dp', 'tensor'), may hold values from -6 to 6
- adapter_down: bfloat16 [2, 4096, 128], P('section', 'tensor'), may hold values from -0.09375 to 0.09375
- adapter_up: bfloat16 [2, 128, 4096], P('section', None, 'tensor'), may hold values from -0.5 to 0.5
- gains: bfloat16 [2, 4096], P('section', 'tensor'), may hold values from 0.25 to 1.75
- head: bfloat16 [4096, 128], P('tensor'), may hold values from -0.375 to 0.375
- labels: int32 [2, 512], P(None, 'dp'), may hold values from 0 to 127
- valid: int32 [2, 512], P(None, 'dp'), may hold values from 0 to 1, as said below
Outputs:
- grads_down: float32 [2, 4096, 128], P('section', 'tensor', 'dp')
- grads_up: float32 [2, 128, 4096], P('section', 'dp', 'tensor')
- grads_gain: float32 [2, 4096], P('section', 'tensor')
The draws below stay inside these ranges and needn't reach their ends.
Inputs may be any that keep to these rules, and one draw needn't show every extreme that they name: In each microbatch the first of every 128 consecutive tokens is valid.
All inputs are finite; a program needn't handle non-finite values.
Results may differ from the reference program's by a relative error of at most 0.015.
Values may be sent and summed in bfloat16 or wider, within the bound.
A program may use at most 64 MiB of HBM per device.

```python
import jax
import jax.numpy as jnp
from jax import lax

D = 4096
RANK = 128
LABELS = 128
TOK_DEV = 128
MICRO = 2
SECTIONS = 2
TOKENS = 512


def draw_valid(key, part):
    column = jnp.arange(TOKENS, dtype=jnp.int32)
    replica = column // TOK_DEV
    groups = TOKENS // TOK_DEV
    threshold = 256 + 512 * replica // max(groups - 1, 1)
    random_bits = jax.random.randint(key, (MICRO, TOKENS), 0, 1024, dtype=jnp.int32)
    chosen = (random_bits < threshold[None, :]) | (column % TOK_DEV == 0)[None, :]
    return chosen.astype(jnp.int32)


def with_ends(values, stream_key, smallest, top_value):
    spot = [jax.random.randint(jax.random.fold_in(stream_key, axis), (), 0, length) for axis, length in enumerate(values.shape)]
    main_axis = values.shape.index(max(values.shape))
    beside = spot[:main_axis] + [(spot[main_axis] + 1) % values.shape[main_axis]] + spot[main_axis + 1:]
    return values.at[tuple(spot)].set(smallest).at[tuple(beside)].set(top_value)


def block_levels(own_key, dims, cuts, low, largest):
    gain = 1.0
    for axis_at, shards_of in cuts:
        steps = jax.random.uniform(jax.random.fold_in(jax.random.fold_in(own_key, 6), axis_at), (shards_of,), jnp.float32, low / len(cuts), largest / len(cuts))
        gain = gain * jnp.repeat(jnp.exp(steps), dims[axis_at] // shards_of).reshape((-1,) + (1,) * (len(dims) - 1 - axis_at))
    return gain


def centred(own_key, extent, width, reach, pieces=(), held_as=jnp.bfloat16):
    entries = jax.random.normal(own_key, extent, jnp.float32) * width
    if len(pieces) > 0:
        entries = block_levels(own_key, extent, pieces, -0.22, 0.18) * entries
    return jnp.clip(entries, min=-reach, max=reach).astype(held_as)


def setup_inputs(seed: int = 0) -> dict:
    key_list = jax.random.split(jax.random.key(seed), 8)
    inputs = centred(key_list[0], (MICRO, TOKENS, D), 1.0, 6.0, ((1, 4), (2, 4)))
    adapter_down = centred(key_list[1], (SECTIONS, D, RANK), D ** -0.5, 0.09375, ((0, 2), (1, 4)))
    adapter_up = centred(key_list[2], (SECTIONS, RANK, D), RANK ** -0.5, 0.5, ((0, 2), (2, 4)))
    gains = jnp.clip(1.0 + 0.15 * jax.random.normal(key_list[3], (SECTIONS, D), jnp.float32), 0.25, 1.75).astype(jnp.bfloat16)
    head = centred(key_list[4], (D, LABELS), (D // 16) ** -0.5, 0.375, ((0, 4),))
    labels = with_ends(jax.random.randint(key_list[5], (MICRO, TOKENS), 0, LABELS), jax.random.fold_in(key_list[5], 1), 0, LABELS - 1).astype(jnp.int32)
    valid = draw_valid(jax.random.fold_in(key_list[7], 71), 0)
    return dict(inputs=inputs, adapter_down=adapter_down, adapter_up=adapter_up, gains=gains, head=head, labels=labels, valid=valid)


epsilon = 1e-05

def layer_forward(inbound, gain_row, down_weight, up_weight):
    values = inbound.astype(jnp.float32)
    squares = lax.optimization_barrier(jnp.sum(values * values, axis=1))
    inverse = lax.rsqrt(squares / D + epsilon)
    scaled = (values * gain_row).astype(jnp.bfloat16)
    projected = jnp.dot(scaled, down_weight, preferred_element_type=jnp.float32)
    hidden = jax.nn.silu(inverse[:, None] * projected).astype(jnp.bfloat16)
    outbound = (values + jnp.dot(hidden, up_weight, preferred_element_type=jnp.float32)).astype(jnp.bfloat16)
    return (outbound, projected, inverse)

def head_backward(final_state, head, label_row, valid_row):
    values = final_state.astype(jnp.float32)
    squares = lax.optimization_barrier(jnp.sum(values * values, axis=1))
    inverse = lax.rsqrt(squares / D + epsilon)
    logit_base = jnp.dot(final_state, head, preferred_element_type=jnp.float32)
    logits = inverse[:, None] * logit_base
    shifted = logits - lax.optimization_barrier(jnp.max(logits, axis=1, keepdims=True))
    expo_terms = jnp.exp(shifted)
    softmax_prob = expo_terms / lax.optimization_barrier(jnp.sum(expo_terms, axis=1, keepdims=True))
    classes = lax.broadcasted_iota(jnp.int32, logits.shape, 1)
    onehot = (classes == label_row[:, None]).astype(jnp.float32)
    cotangent = (softmax_prob - onehot) * valid_row[:, None].astype(jnp.float32)
    radial = lax.optimization_barrier(jnp.sum(cotangent * logit_base, axis=1))
    weighted = (inverse[:, None] * cotangent).astype(jnp.bfloat16)
    back_term = jnp.dot(weighted, head.T, preferred_element_type=jnp.float32)
    result = back_term - (inverse ** 3 / D * radial)[:, None] * values
    return result.astype(jnp.bfloat16)

def layer_backward(cotangent, inbound, projected, inverse, gain_row, down_weight, up_weight):
    hidden_grad = jnp.dot(cotangent, up_weight.T, preferred_element_type=jnp.float32)
    pre_act = inverse[:, None] * projected
    sigmoid_val = jax.nn.sigmoid(pre_act)
    act_grad = hidden_grad * sigmoid_val * (1.0 + pre_act * (1.0 - sigmoid_val))
    radial = lax.optimization_barrier(jnp.sum(act_grad * projected, axis=1))
    weighted = (inverse[:, None] * act_grad).astype(jnp.bfloat16)
    scaled_grad = jnp.dot(weighted, down_weight.T, preferred_element_type=jnp.float32)
    values = inbound.astype(jnp.float32)
    outbound = (cotangent.astype(jnp.float32) + gain_row * scaled_grad - (inverse ** 3 / D * radial)[:, None] * values).astype(jnp.bfloat16)
    scaled = (values * gain_row).astype(jnp.bfloat16)
    hidden = jax.nn.silu(pre_act).astype(jnp.bfloat16)
    down_grad = jnp.dot(scaled.T, weighted, preferred_element_type=jnp.float32)
    up_grad = jnp.dot(hidden.T, cotangent, preferred_element_type=jnp.float32)
    gain_grad = lax.optimization_barrier(jnp.sum(scaled_grad * values, axis=0))
    return (outbound, down_grad, up_grad, gain_grad)

def reference(inputs, adapter_down, adapter_up, gains, head, labels, valid):
    down_sums = [jnp.zeros((D, RANK), jnp.float32) for layer in range(SECTIONS)]
    up_sums = [jnp.zeros((RANK, D), jnp.float32) for layer in range(SECTIONS)]
    gain_sums = [jnp.zeros((D,), jnp.float32) for layer in range(SECTIONS)]
    for micro_index in range(MICRO):
        state = inputs[micro_index]
        saved = []
        for layer in range(SECTIONS):
            outbound, projected, inverse = layer_forward(state, gains[layer].astype(jnp.float32), adapter_down[layer], adapter_up[layer])
            saved.append((state, projected, inverse))
            state = outbound
        cotangent = head_backward(state, head, labels[micro_index], valid[micro_index])
        for layer in reversed(range(SECTIONS)):
            inbound, projected, inverse = saved[layer]
            cotangent, down_grad, up_grad, gain_grad = layer_backward(cotangent, inbound, projected, inverse, gains[layer].astype(jnp.float32), adapter_down[layer], adapter_up[layer])
            down_sums[layer] = down_sums[layer] + down_grad
            up_sums[layer] = up_sums[layer] + up_grad
            gain_sums[layer] = gain_sums[layer] + gain_grad
    total_count = jnp.sum(valid.astype(jnp.float32))
    return (jnp.stack(down_sums) / total_count, jnp.stack(up_sums) / total_count, jnp.stack(gain_sums) / total_count)
```

```python
import functools

import jax
import jax.numpy as jnp
from jax import lax
from jax.experimental import pallas as pl
from jax.experimental.pallas import tpu as pltpu
from jax.sharding import PartitionSpec as P

MESH = pl.DeviceIdType.MESH
epsilon = 1e-05
F32 = jnp.float32
BF16 = jnp.bfloat16


def mm(a, b):
    return jnp.dot(a, b, preferred_element_type=F32)


def mm_nt(a, b):
    return lax.dot_general(a, b, (((1,), (1,)), ((), ())), preferred_element_type=F32)


def mm_tn(a, b):
    return lax.dot_general(a, b, (((0,), (0,)), ((), ())), preferred_element_type=F32)


def split(v):
    high = v.astype(BF16)
    return high, (v - high.astype(F32)).astype(BF16)


def kernel(
    nt, nd, width,
    x_ref, dn_ref, up_ref, gain_ref, head_ref, lab_ref, val_ref,
    down_out, up_out, gain_out,
    odn, oup, ogain, stok, rtok, sgram, rgram, pgram, gall, sres, res, sdp, rdp, sgn, rgn,
    sib_s, sib_r, tok_s, tok_r, gr_s, gr_r, ga_s, ga_r, re_s, re_r, dp_s, dp_r,
):
    s, d, t = lax.axis_index("section"), lax.axis_index("dp"), lax.axis_index("tensor")
    first = s == 0
    tokens, feats = x_ref.shape
    rank = dn_ref.shape[1]
    half = tokens // 2
    own = half // nt
    rows = rank // nt
    part = rank // nd
    wire = stok.dtype

    def peer(k, other):
        return (1 - s if other else s, d, lax.rem(t + k, nt))

    group = [(k, o) for k in range(nt) for o in (0, 1) if (k, o) != (0, 0)]

    barrier = pltpu.get_barrier_semaphore()
    for k, o in group:
        pl.semaphore_signal(barrier, inc=1, device_id=peer(k, o), device_id_type=MESH)
    for k in range(1, nd):
        pl.semaphore_signal(barrier, inc=1, device_id=(s, lax.rem(d + k, nd), t), device_id_type=MESH)
    pl.semaphore_wait(barrier, len(group) + nd - 1)

    def send(src, dst, ss, rs, to):
        copy = pltpu.make_async_remote_copy(
            src_ref=src, dst_ref=dst, send_sem=ss, recv_sem=rs, device_id=to, device_id_type=MESH
        )
        copy.start()
        return copy

    started = []
    sib = [
        send(a, b, sib_s.at[i], sib_r.at[i], peer(0, 1))
        for i, (a, b) in enumerate(((up_ref, oup), (dn_ref, odn), (gain_ref, ogain)))
    ]
    started += sib

    gain = gain_ref[...].astype(F32)
    up = up_ref[...]
    head = head_ref[...]
    gram_a = mm_nt(up, up)
    gram_b = mm(up, head)
    sib[0].wait_recv()
    gram_c = mm_nt(up, oup[...])
    scaled_other = (oup[...].astype(F32) * gain).astype(BF16)
    gram_d = mm(scaled_other, dn_ref[...])
    gram_c = jnp.where(first, gram_c, gram_d)
    for j, g in enumerate((gram_a, gram_b, gram_c)):
        g = g.astype(wire)
        for i in range(nt):
            sgram[i, j] = g[i * rows : (i + 1) * rows]
    gram_copies = []
    for k in range(1, nt):
        gram_copies.append(
            send(sgram.at[lax.rem(t + k, nt)], rgram.at[k], gr_s.at[k], gr_r.at[k], peer(k, 0))
        )
    started += gram_copies

    xb = x_ref[...]
    xf = xb.astype(F32)
    proj = mm((xf * gain).astype(BF16), dn_ref[...]).astype(wire)
    xup = mm_nt(xb, up).astype(wire)
    for b in range(2):
        for i in range(nt):
            at = b * half + i * own
            stok[b, i, 0] = proj[at : at + own]
            stok[b, i, 1] = xup[at : at + own]
    tok_copies = {}
    for k in range(nt):
        to = lax.rem(t + k, nt)
        tok_copies[k, 1] = send(
            stok.at[1 - s, to, pl.ds(0, 2)], rtok.at[1, k, pl.ds(0, 2)],
            tok_s.at[1, k], tok_r.at[1, k], peer(k, 1),
        )
    xm = x_ref[pl.ds(pl.multiple_of(s * half, half), half), :]
    xmf = xm.astype(F32)
    xhead = mm(xm, head)
    squares = jnp.broadcast_to(jnp.sum(xmf * xmf, axis=1, keepdims=True), (half, rank))
    hh, hl = split(xhead)
    qh, ql = split(squares)
    lane_h = lax.broadcasted_iota(jnp.int32, (half, rank), 1)
    q = jnp.where(lane_h < rank // 2, qh.astype(F32), ql.astype(F32)).astype(wire)
    hh, hl = hh.astype(wire), hl.astype(wire)
    for i in range(nt):
        stok[s, i, 2] = hh[i * own : (i + 1) * own]
        stok[s, i, 3] = hl[i * own : (i + 1) * own]
        stok[s, i, 4] = q[i * own : (i + 1) * own]
    for k in range(1, nt):
        to = lax.rem(t + k, nt)
        tok_copies[k, 0] = send(
            stok.at[s, to], rtok.at[0, k], tok_s.at[0, k], tok_r.at[0, k], peer(k, 0)
        )
    started += list(tok_copies.values())

    total = sgram[t].astype(F32)
    for k in range(1, nt):
        gram_copies[k - 1].wait_recv()
        total = total + rgram[k].astype(F32)
    total = total.astype(wire)
    pgram[...] = total
    gall[s, t] = total
    all_copies = [
        send(pgram, gall.at[s, t], ga_s.at[o, k], ga_r.at[o, k], peer(k, o)) for k, o in group
    ]
    started += all_copies

    lab = jnp.where(first, lab_ref[0:1, :], lab_ref[1:2, :])
    val = jnp.where(first, val_ref[0:1, :], val_ref[1:2, :]).astype(F32)
    labels_n = head.shape[1]
    hot_t = jnp.where(lax.broadcasted_iota(jnp.int32, (labels_n, half), 0) == lab, val, 0.0).astype(BF16)
    val_t = jnp.broadcast_to(val, (labels_n, half)).astype(BF16)
    pick = (
        lax.broadcasted_iota(jnp.int32, (own, half), 0) + t * own
        == lax.broadcasted_iota(jnp.int32, (own, half), 1)
    ).astype(F32).astype(BF16)
    onehot = mm_nt(pick, hot_t)
    validity = mm_nt(pick, val_t)
    count = jnp.sum(val_ref[...].astype(F32))

    mine = stok[s, t].astype(F32)
    for k in range(1, nt):
        tok_copies[k, 0].wait_recv()
        mine = mine + rtok[0, k].astype(F32)
    tok_copies[0, 1].wait_recv()
    theirs = rtok[1, 0, 0:2].astype(F32)
    for k in range(1, nt):
        tok_copies[k, 1].wait_recv()
        theirs = theirs + rtok[1, k, 0:2].astype(F32)
    p0 = jnp.where(first, mine[0], theirs[0])
    p1 = jnp.where(first, theirs[0], mine[0])
    v0 = jnp.where(first, mine[1], theirs[1])
    v1 = jnp.where(first, theirs[1], mine[1])
    xh = mine[2] + mine[3]
    sq0 = mine[4][:, 0:1] + mine[4][:, rank // 2 : rank // 2 + 1]

    for c in all_copies:
        c.wait_recv()

    def gram(a, j):
        return gall[a, :, j].reshape(rank, rank).astype(BF16)

    a0, b0, c0 = gram(0, 0), gram(0, 1), gram(0, 2)
    a1, b1, d1 = gram(1, 0), gram(1, 1), gram(1, 2)

    def rowsum(v):
        return jnp.sum(v, axis=1, keepdims=True)

    inv0 = lax.rsqrt(sq0 / width + epsilon)
    pre0 = inv0 * p0
    sig0 = jax.nn.sigmoid(pre0)
    h0 = (pre0 * sig0).astype(BF16)
    h0f = h0.astype(F32)
    h0a = mm(h0, a0)
    p1 = p1 + mm(h0, d1)
    s1u0 = v0 + h0a
    s1u1 = v1 + mm(h0, c0)
    base = xh + mm(h0, b0)
    sq1 = sq0 + rowsum(h0f * (v0 + s1u0))
    inv1 = lax.rsqrt(sq1 / width + epsilon)
    pre1 = inv1 * p1
    sig1 = jax.nn.sigmoid(pre1)
    h1 = (pre1 * sig1).astype(BF16)
    h1f = h1.astype(F32)
    yu1 = s1u1 + mm(h1, a1)
    yu0 = s1u0 + mm_nt(h1, c0)
    base = base + mm(h1, b1)
    sq2 = sq1 + rowsum(h1f * (s1u1 + yu1))
    inv2 = lax.rsqrt(sq2 / width + epsilon)
    logits = inv2 * base
    expo = jnp.exp(logits - jnp.max(logits, axis=1, keepdims=True))
    cot = expo / rowsum(expo) * validity - onehot
    radial = rowsum(cot * base)
    wh = (inv2 * cot).astype(BF16)
    ch = inv2 * inv2 * inv2 / width * radial
    hg1 = mm_nt(wh, b1) - ch * yu1
    act1 = hg1 * sig1 * (1.0 + pre1 * (1.0 - sig1))
    w1 = (inv1 * act1).astype(BF16)
    c1 = inv1 * inv1 * inv1 / width * rowsum(act1 * p1)
    hg0 = mm_nt(wh, b0) - ch * yu0 + mm_nt(w1, d1) - c1 * s1u0
    act0 = hg0 * sig0 * (1.0 + pre0 * (1.0 - sig0))
    w0 = (inv0 * act0).astype(BF16)

    ch_h, ch_l = split(ch)
    c1_h, c1_l = split(c1)
    lane = lax.broadcasted_iota(jnp.int32, (own, rank), 1)
    q4 = rank // 4
    coef = jnp.where(
        lane < q4, ch_h.astype(F32),
        jnp.where(lane < 2 * q4, ch_l.astype(F32), jnp.where(lane < 3 * q4, c1_h.astype(F32), c1_l.astype(F32))),
    )
    for j, v in enumerate((h0, h1, w0, w1, wh, coef)):
        v = v.astype(wire)
        sres[j] = v
        res[s, t, j] = v
    res_copies = [
        send(sres, res.at[s, t], re_s.at[o, k], re_r.at[o, k], peer(k, o)) for k, o in group
    ]
    started += res_copies
    sib[1].wait_recv()
    sib[2].wait_recv()
    for c in res_copies:
        c.wait_recv()

    def got(j):
        return res[:, :, j].reshape(tokens, res.shape[-1])

    dp_copies = []

    def piece(j, full):
        full = full.astype(BF16)
        for i in range(nd):
            sdp[i, j] = full[i * part : (i + 1) * part]

    def finish(state, own_w, own_h, cotangent):
        scaled = (state * gain).astype(BF16)
        piece(0, mm_tn(own_w, scaled))
        gain_row = jnp.sum(mm_nt(own_w, dn_ref[...]) * state, axis=0, keepdims=True)
        sgn[0:1, :] = gain_row
        sgn[1:2, :] = jnp.full((1, feats), count, F32)
        piece(1, mm_tn(own_h, cotangent().astype(BF16)))

    h0g, h1g, w1g, whg = (got(j).astype(BF16) for j in (0, 1, 3, 4))
    cg = got(5).astype(F32)
    chg = cg[:, 0:1] + cg[:, q4 : q4 + 1]
    c1g = cg[:, 2 * q4 : 2 * q4 + 1] + cg[:, 3 * q4 : 3 * q4 + 1]

    @pl.when(s == 0)
    def _():
        def cotangent():
            s1 = xf + mm(h0g, up)
            y = s1 + mm(h1g, oup[...])
            g2 = mm_nt(whg, head) - chg * y
            return g2 + ogain[...].astype(F32) * mm_nt(w1g, odn[...]) - c1g * s1

        finish(xf, got(2).astype(BF16), h0g, cotangent)

    @pl.when(s != 0)
    def _():
        s1 = xf + mm(h0g, oup[...])

        def cotangent():
            y = s1 + mm(h1g, up)
            return mm_nt(whg, head) - chg * y

        finish(s1, w1g, h1g, cotangent)

    for k in range(1, nd):
        to = (s, lax.rem(d + k, nd), t)
        dp_copies.append((
            send(sdp.at[lax.rem(d + k, nd)], rdp.at[k], dp_s.at[0, k], dp_r.at[0, k], to),
            send(sgn, rgn.at[k], dp_s.at[1, k], dp_r.at[1, k], to),
        ))
    sums = sdp[d].astype(F32)
    small = sgn[...]
    for big, little in dp_copies:
        started += [big, little]
    for k in range(1, nd):
        dp_copies[k - 1][1].wait_recv()
        small = small + rgn[k]
        dp_copies[k - 1][0].wait_recv()
        sums = sums + rdp[k].astype(F32)
    scale = 1.0 / small[1:2, :]
    gain_out[...] = small[0:1, :] * scale
    up_out[...] = sums[1] * scale
    down_out[...] = sums[0] * scale
    for c in started:
        c.wait_send()


def solution(mesh):
    nt, nd, ns = mesh.shape["tensor"], mesh.shape["dp"], mesh.shape["section"]
    assert ns == 2

    def local(inputs, down, up, gains, head, labels, valid):
        micro, per, feats = inputs.shape
        assert micro == ns
        tokens = micro * per
        rank = down.shape[2]
        own, rows, part = tokens // ns // nt, rank // nt, rank // nd
        wire = BF16 if own % 16 == 0 and rows % 16 == 0 else F32
        vmem = pl.BlockSpec(memory_space=pltpu.VMEM)
        dma = pltpu.SemaphoreType.DMA
        down_t, up_g, gain_g = pl.pallas_call(
            functools.partial(kernel, nt, nd, feats * nt),
            out_shape=(
                jax.ShapeDtypeStruct((part, feats), F32),
                jax.ShapeDtypeStruct((part, feats), F32),
                jax.ShapeDtypeStruct((1, feats), F32),
            ),
            in_specs=[vmem] * 7,
            out_specs=(vmem,) * 3,
            scratch_shapes=[
                pltpu.VMEM((feats, rank), BF16),
                pltpu.VMEM((rank, feats), BF16),
                pltpu.VMEM((1, feats), BF16),
                pltpu.VMEM((2, nt, 5, own, rank), wire),
                pltpu.VMEM((2, nt, 5, own, rank), wire),
                pltpu.VMEM((nt, 3, rows, rank), wire),
                pltpu.VMEM((nt, 3, rows, rank), wire),
                pltpu.VMEM((3, rows, rank), wire),
                pltpu.VMEM((2, nt, 3, rows, rank), wire),
                pltpu.VMEM((6, own, rank), wire),
                pltpu.VMEM((2, nt, 6, own, rank), wire),
                pltpu.VMEM((nd, 2, part, feats), BF16),
                pltpu.VMEM((nd, 2, part, feats), BF16),
                pltpu.VMEM((2, feats), F32),
                pltpu.VMEM((nd, 2, feats), F32),
                dma((3,)), dma((3,)),
                dma((2, nt)), dma((2, nt)),
                dma((nt,)), dma((nt,)),
                dma((2, nt)), dma((2, nt)),
                dma((2, nt)), dma((2, nt)),
                dma((2, nd)), dma((2, nd)),
            ],
            compiler_params=pltpu.CompilerParams(collective_id=0, has_side_effects=True),
        )(inputs.reshape(tokens, feats), down[0], up[0], gains, head, labels, valid)
        return down_t.T[None], up_g[None], gain_g

    return jax.shard_map(
        local,
        mesh=mesh,
        in_specs=(
            P(None, "dp", "tensor"),
            P("section", "tensor", None),
            P("section", None, "tensor"),
            P("section", "tensor"),
            P("tensor", None),
            P(None, "dp"),
            P(None, "dp"),
        ),
        out_specs=(
            P("section", "tensor", "dp"),
            P("section", "dp", "tensor"),
            P("section", "tensor"),
        ),
        check_vma=False,
    )
```

```python
import functools

import jax
import jax.numpy as jnp
from jax import lax
from jax.experimental import pallas as pl
from jax.experimental.pallas import tpu as pltpu
from jax.sharding import PartitionSpec as P

MESH = pl.DeviceIdType.MESH
epsilon = 1e-05
F32 = jnp.float32
BF16 = jnp.bfloat16


def mm(a, b):
    return jnp.dot(a, b, preferred_element_type=F32)


def mm_nt(a, b):
    return lax.dot_general(a, b, (((1,), (1,)), ((), ())), preferred_element_type=F32)


def mm_tn(a, b):
    return lax.dot_general(a, b, (((0,), (0,)), ((), ())), preferred_element_type=F32)


def split(v):
    high = v.astype(BF16)
    return high, (v - high.astype(F32)).astype(BF16)


def kernel(
    nt, nd, width,
    x_hbm, dn_hbm, up_hbm, gain_hbm, head_hbm, lab_hbm, val_hbm,
    out,
    x_ref, dn_ref, up_ref, gain_ref, head_ref, lab_ref, val_ref,
    odn, oup, ogain, stok, rtok, sgram, rgram, pgram, gall, sres, res, sdp, rdp, sgn, rgn,
    load, sib_s, sib_r, tok_s, tok_r, gr_s, gr_r, ga_s, ga_r, re_s, re_r, fw_s, fw_r, dp_s, dp_r,
):
    s, d, t = lax.axis_index("section"), lax.axis_index("dp"), lax.axis_index("tensor")
    first = s == 0
    tokens, feats = x_ref.shape
    rank = dn_ref.shape[1]
    half = tokens // 2
    own = half // nt
    rows = rank // nt
    part = rank // nd
    wire = stok.dtype

    def peer(k, other):
        return (1 - s if other else s, d, lax.rem(t + k, nt))

    group = [(k, o) for k in range(nt) for o in (0, 1) if (k, o) != (0, 0)]

    loads = [
        pltpu.make_async_copy(a, b, load.at[i])
        for i, (a, b) in enumerate((
            (up_hbm, up_ref), (head_hbm, head_ref), (x_hbm, x_ref), (gain_hbm, gain_ref),
            (dn_hbm, dn_ref), (lab_hbm, lab_ref), (val_hbm, val_ref),
        ))
    ]
    for c in loads:
        c.start()

    barrier = pltpu.get_barrier_semaphore()
    for k, o in group:
        pl.semaphore_signal(barrier, inc=1, device_id=peer(k, o), device_id_type=MESH)
    for k in range(1, nd):
        pl.semaphore_signal(barrier, inc=1, device_id=(s, lax.rem(d + k, nd), t), device_id_type=MESH)

    def send(src, dst, ss, rs, to):
        copy = pltpu.make_async_remote_copy(
            src_ref=src, dst_ref=dst, send_sem=ss, recv_sem=rs, device_id=to, device_id_type=MESH
        )
        copy.start()
        return copy

    def put_gram(j, g):
        g = g.astype(wire)
        for i in range(nt):
            sgram[i, j] = g[i * rows : (i + 1) * rows]

    loads[0].wait()
    up = up_ref[...]
    put_gram(0, mm_nt(up, up))
    loads[1].wait()
    head = head_ref[...]
    put_gram(1, mm(up, head))
    for c in loads[2:]:
        c.wait()
    gain = gain_ref[...].astype(F32)
    xb = x_ref[...]
    xf = xb.astype(F32)
    xup = mm_nt(xb, up).astype(wire)
    proj = mm((xf * gain).astype(BF16), dn_ref[...]).astype(wire)
    for b in range(2):
        for i in range(nt):
            at = b * half + i * own
            stok[b, i, 0] = proj[at : at + own]
            stok[b, i, 1] = xup[at : at + own]

    pl.semaphore_wait(barrier, len(group) + nd - 1)

    sib = [
        send(a, b, sib_s.at[i], sib_r.at[i], peer(0, 1))
        for i, (a, b) in enumerate(((up_ref, oup), (dn_ref, odn), (gain_ref, ogain)))
    ]
    started = list(sib)
    spans = (pl.ds(0, 2), pl.ds(2, 1))

    def scatter_gram(j):
        copies = [
            send(
                sgram.at[lax.rem(t + k, nt), spans[j]], rgram.at[k, spans[j]],
                gr_s.at[j, k], gr_r.at[j, k], peer(k, 0),
            )
            for k in range(1, nt)
        ]
        started.extend(copies)
        return copies

    def gather_gram(j, copies):
        total = sgram[t, spans[j]].astype(F32)
        for k in range(1, nt):
            copies[k - 1].wait_recv()
            total = total + rgram[k, spans[j]].astype(F32)
        total = total.astype(wire)
        pgram[spans[j]] = total
        gall[s, t, spans[j]] = total
        out_copies = [
            send(
                pgram.at[spans[j]], gall.at[s, t, spans[j]],
                ga_s.at[j, o, k], ga_r.at[j, o, k], peer(k, o),
            )
            for k, o in group
        ]
        started.extend(out_copies)
        return out_copies

    ab_copies = scatter_gram(0)
    tok_copies = {}
    for k in range(nt):
        to = lax.rem(t + k, nt)
        tok_copies[k, 1] = send(
            stok.at[1 - s, to, pl.ds(0, 2)], rtok.at[1, k, pl.ds(0, 2)],
            tok_s.at[1, k], tok_r.at[1, k], peer(k, 1),
        )
    xm = x_ref[pl.ds(pl.multiple_of(s * half, half), half), :]
    xmf = xm.astype(F32)
    xhead = mm(xm, head)
    squares = jnp.broadcast_to(jnp.sum(xmf * xmf, axis=1, keepdims=True), (half, rank))
    hh, hl = split(xhead)
    qh, ql = split(squares)
    lane_h = lax.broadcasted_iota(jnp.int32, (half, rank), 1)
    q = jnp.where(lane_h < rank // 2, qh.astype(F32), ql.astype(F32)).astype(wire)
    hh, hl = hh.astype(wire), hl.astype(wire)
    for i in range(nt):
        stok[s, i, 2] = hh[i * own : (i + 1) * own]
        stok[s, i, 3] = hl[i * own : (i + 1) * own]
        stok[s, i, 4] = q[i * own : (i + 1) * own]

    sib[0].wait_recv()
    gram_c = mm_nt(up, oup[...])
    gram_d = mm((oup[...].astype(F32) * gain).astype(BF16), dn_ref[...])
    put_gram(2, jnp.where(first, gram_c, gram_d))
    c_copies = scatter_gram(1)
    for k in range(1, nt):
        to = lax.rem(t + k, nt)
        tok_copies[k, 0] = send(
            stok.at[s, to], rtok.at[0, k], tok_s.at[0, k], tok_r.at[0, k], peer(k, 0)
        )
    started += list(tok_copies.values())
    all_copies = gather_gram(0, ab_copies)
    all_copies = all_copies + gather_gram(1, c_copies)

    lab = jnp.where(first, lab_ref[0:1, :], lab_ref[1:2, :])
    val = jnp.where(first, val_ref[0:1, :], val_ref[1:2, :]).astype(F32)
    labels_n = head.shape[1]
    hot_t = jnp.where(lax.broadcasted_iota(jnp.int32, (labels_n, half), 0) == lab, val, 0.0).astype(BF16)
    val_t = jnp.broadcast_to(val, (labels_n, half)).astype(BF16)
    pick = (
        lax.broadcasted_iota(jnp.int32, (own, half), 0) + t * own
        == lax.broadcasted_iota(jnp.int32, (own, half), 1)
    ).astype(F32).astype(BF16)
    onehot = mm_nt(pick, hot_t)
    validity = mm_nt(pick, val_t)
    count = jnp.sum(val_ref[...].astype(F32))

    mine = stok[s, t].astype(F32)
    for k in range(1, nt):
        tok_copies[k, 0].wait_recv()
        mine = mine + rtok[0, k].astype(F32)
    tok_copies[0, 1].wait_recv()
    theirs = rtok[1, 0, 0:2].astype(F32)
    for k in range(1, nt):
        tok_copies[k, 1].wait_recv()
        theirs = theirs + rtok[1, k, 0:2].astype(F32)
    p0 = jnp.where(first, mine[0], theirs[0])
    p1 = jnp.where(first, theirs[0], mine[0])
    v0 = jnp.where(first, mine[1], theirs[1])
    v1 = jnp.where(first, theirs[1], mine[1])
    xh = mine[2] + mine[3]
    sq0 = mine[4][:, 0:1] + mine[4][:, rank // 2 : rank // 2 + 1]

    for c in all_copies:
        c.wait_recv()

    def gram(a, j):
        return gall[a, :, j].reshape(rank, rank).astype(BF16)

    a0, b0, c0 = gram(0, 0), gram(0, 1), gram(0, 2)
    a1, b1, d1 = gram(1, 0), gram(1, 1), gram(1, 2)

    def rowsum(v):
        return jnp.sum(v, axis=1, keepdims=True)

    inv0 = lax.rsqrt(sq0 / width + epsilon)
    pre0 = inv0 * p0
    sig0 = jax.nn.sigmoid(pre0)
    h0 = (pre0 * sig0).astype(BF16)
    h0f = h0.astype(F32)
    h0a = mm(h0, a0)
    p1 = p1 + mm(h0, d1)
    s1u0 = v0 + h0a
    s1u1 = v1 + mm(h0, c0)
    base = xh + mm(h0, b0)
    sq1 = sq0 + rowsum(h0f * (v0 + s1u0))
    inv1 = lax.rsqrt(sq1 / width + epsilon)
    pre1 = inv1 * p1
    sig1 = jax.nn.sigmoid(pre1)
    h1 = (pre1 * sig1).astype(BF16)
    h1f = h1.astype(F32)
    yu1 = s1u1 + mm(h1, a1)
    yu0 = s1u0 + mm_nt(h1, c0)
    base = base + mm(h1, b1)
    sq2 = sq1 + rowsum(h1f * (s1u1 + yu1))
    inv2 = lax.rsqrt(sq2 / width + epsilon)
    logits = inv2 * base
    expo = jnp.exp(logits - jnp.max(logits, axis=1, keepdims=True))
    cot = expo / rowsum(expo) * validity - onehot
    radial = rowsum(cot * base)
    wh = (inv2 * cot).astype(BF16)
    ch = inv2 * inv2 * inv2 / width * radial
    hg1 = mm_nt(wh, b1) - ch * yu1
    act1 = hg1 * sig1 * (1.0 + pre1 * (1.0 - sig1))
    w1 = (inv1 * act1).astype(BF16)
    c1 = inv1 * inv1 * inv1 / width * rowsum(act1 * p1)
    hg0 = mm_nt(wh, b0) - ch * yu0 + mm_nt(w1, d1) - c1 * s1u0
    act0 = hg0 * sig0 * (1.0 + pre0 * (1.0 - sig0))
    w0 = (inv0 * act0).astype(BF16)

    ch_h, ch_l = split(ch)
    c1_h, c1_l = split(c1)
    lane = lax.broadcasted_iota(jnp.int32, (own, rank), 1)
    q4 = rank // 4
    coef = jnp.where(
        lane < q4, ch_h.astype(F32),
        jnp.where(lane < 2 * q4, ch_l.astype(F32), jnp.where(lane < 3 * q4, c1_h.astype(F32), c1_l.astype(F32))),
    )
    for j, v in enumerate((h0, h1, w0, w1, wh, coef)):
        v = v.astype(wire)
        sres[j] = v
        res[s, t, j] = v
    res_copies = {
        k: send(sres, res.at[s, t], re_s.at[k], re_r.at[k], peer(k, 0 if k else 1)) for k in range(nt)
    }
    forwards = []
    for k in range(1, nt):
        res_copies[k].wait_recv()
        at = lax.rem(t + nt - k, nt)
        forwards.append(send(res.at[s, at], res.at[s, at], fw_s.at[k], fw_r.at[k], peer(0, 1)))
    started += list(res_copies.values()) + forwards
    sib[1].wait_recv()
    sib[2].wait_recv()
    res_copies[0].wait_recv()
    for c in forwards:
        c.wait_recv()

    def got(j):
        return res[:, :, j].reshape(tokens, res.shape[-1])

    def piece(j, full):
        full = full.astype(BF16)
        for i in range(nd):
            sdp[i, j] = full[i * part : (i + 1) * part]
        for k in range(1, nd):
            dp_copy(j, k).start()

    def dp_copy(j, k):
        to = lax.rem(d + k, nd)
        return pltpu.make_async_remote_copy(
            src_ref=sdp.at[to, j], dst_ref=rdp.at[k, j], send_sem=dp_s.at[j, k], recv_sem=dp_r.at[j, k],
            device_id=(s, to, t), device_id_type=MESH,
        )

    def finish(state, own_w, own_h, cotangent):
        scaled = (state * gain).astype(BF16)
        piece(0, mm_tn(own_w, scaled))
        gain_row = jnp.sum(mm_nt(own_w, dn_ref[...]) * state, axis=0, keepdims=True)
        sgn[0:1, :] = gain_row
        sgn[1:2, :] = jnp.full((1, feats), count, F32)
        piece(1, mm_tn(own_h, cotangent().astype(BF16)))

    h0g, h1g, w1g, whg = (got(j).astype(BF16) for j in (0, 1, 3, 4))
    cg = got(5).astype(F32)
    chg = cg[:, 0:1] + cg[:, q4 : q4 + 1]
    c1g = cg[:, 2 * q4 : 2 * q4 + 1] + cg[:, 3 * q4 : 3 * q4 + 1]

    @pl.when(s == 0)
    def _():
        def cotangent():
            s1 = xf + mm(h0g, up)
            y = s1 + mm(h1g, oup[...])
            g2 = mm_nt(whg, head) - chg * y
            return g2 + ogain[...].astype(F32) * mm_nt(w1g, odn[...]) - c1g * s1

        finish(xf, got(2).astype(BF16), h0g, cotangent)

    @pl.when(s != 0)
    def _():
        s1 = xf + mm(h0g, oup[...])

        def cotangent():
            y = s1 + mm(h1g, up)
            return mm_nt(whg, head) - chg * y

        finish(s1, w1g, h1g, cotangent)

    small_copies = [
        send(sgn, rgn.at[k], dp_s.at[2, k], dp_r.at[2, k], (s, lax.rem(d + k, nd), t)) for k in range(1, nd)
    ]
    started += small_copies
    small = sgn[...]
    for k in range(1, nd):
        small_copies[k - 1].wait_recv()
        small = small + rgn[k]
    out[2 * part : 2 * part + 2, :] = small
    for j in range(2):
        sums = sdp[d, j].astype(F32)
        for k in range(1, nd):
            dp_copy(j, k).wait_recv()
            sums = sums + rdp[k, j].astype(F32)
        out[j * part : (j + 1) * part, :] = sums
    for j in range(2):
        for k in range(1, nd):
            dp_copy(j, k).wait_send()
    for c in started:
        c.wait_send()


def scale_kernel(part, sums, down_out, up_out, gain_out):
    scale = 1.0 / sums[2 * part + 1 : 2 * part + 2, :]
    down_out[...] = sums[0:part, :] * scale
    up_out[...] = sums[part : 2 * part, :] * scale
    gain_out[...] = sums[2 * part : 2 * part + 1, :] * scale


def solution(mesh):
    nt, nd, ns = mesh.shape["tensor"], mesh.shape["dp"], mesh.shape["section"]
    assert ns == 2

    def local(inputs, down, up, gains, head, labels, valid):
        micro, per, feats = inputs.shape
        assert micro == ns
        tokens = micro * per
        rank = down.shape[2]
        own, rows, part = tokens // ns // nt, rank // nt, rank // nd
        wire = BF16 if own % 16 == 0 and rows % 16 == 0 else F32
        vmem = pl.BlockSpec(memory_space=pltpu.VMEM)
        dma = pltpu.SemaphoreType.DMA
        anyspace = pl.BlockSpec(memory_space=pl.ANY)
        sums = pl.pallas_call(
            functools.partial(kernel, nt, nd, feats * nt),
            out_shape=jax.ShapeDtypeStruct((2 * part + 8, feats), F32),
            in_specs=[anyspace] * 7,
            out_specs=vmem,
            scratch_shapes=[
                pltpu.VMEM((tokens, feats), BF16),
                pltpu.VMEM((feats, rank), BF16),
                pltpu.VMEM((rank, feats), BF16),
                pltpu.VMEM((1, feats), BF16),
                pltpu.VMEM((feats, head.shape[1]), BF16),
                pltpu.VMEM((micro, per), jnp.int32),
                pltpu.VMEM((micro, per), jnp.int32),
                pltpu.VMEM((feats, rank), BF16),
                pltpu.VMEM((rank, feats), BF16),
                pltpu.VMEM((1, feats), BF16),
                pltpu.VMEM((2, nt, 5, own, rank), wire),
                pltpu.VMEM((2, nt, 5, own, rank), wire),
                pltpu.VMEM((nt, 3, rows, rank), wire),
                pltpu.VMEM((nt, 3, rows, rank), wire),
                pltpu.VMEM((3, rows, rank), wire),
                pltpu.VMEM((2, nt, 3, rows, rank), wire),
                pltpu.VMEM((6, own, rank), wire),
                pltpu.VMEM((2, nt, 6, own, rank), wire),
                pltpu.VMEM((nd, 2, part, feats), BF16),
                pltpu.VMEM((nd, 2, part, feats), BF16),
                pltpu.VMEM((2, feats), F32),
                pltpu.VMEM((nd, 2, feats), F32),
                dma((7,)),
                dma((3,)), dma((3,)),
                dma((2, nt)), dma((2, nt)),
                dma((2, nt)), dma((2, nt)),
                dma((2, 2, nt)), dma((2, 2, nt)),
                dma((nt,)), dma((nt,)),
                dma((nt,)), dma((nt,)),
                dma((3, nd)), dma((3, nd)),
            ],
            compiler_params=pltpu.CompilerParams(collective_id=0, has_side_effects=True),
        )(inputs.reshape(tokens, feats), down[0], up[0], gains, head, labels, valid)
        down_t, up_g, gain_g = pl.pallas_call(
            functools.partial(scale_kernel, part),
            out_shape=(
                jax.ShapeDtypeStruct((part, feats), F32),
                jax.ShapeDtypeStruct((part, feats), F32),
                jax.ShapeDtypeStruct((1, feats), F32),
            ),
            in_specs=[vmem],
            out_specs=(vmem,) * 3,
        )(sums)
        return down_t.T[None], up_g[None], gain_g

    return jax.shard_map(
        local,
        mesh=mesh,
        in_specs=(
            P(None, "dp", "tensor"),
            P("section", "tensor", None),
            P("section", None, "tensor"),
            P("section", "tensor"),
            P("tensor", None),
            P(None, "dp"),
            P(None, "dp"),
        ),
        out_specs=(
            P("section", "tensor", "dp"),
            P("section", "dp", "tensor"),
            P("section", "tensor"),
        ),
        check_vma=False,
    )
```

```python
import functools

import jax
import jax.numpy as jnp
from jax import lax
from jax.experimental import pallas as pl
from jax.experimental.pallas import tpu as pltpu
from jax.sharding import PartitionSpec as P

MESH = pl.DeviceIdType.MESH
epsilon = 1e-05
F32 = jnp.float32
BF16 = jnp.bfloat16


def mm(a, b):
    return jnp.dot(a, b, preferred_element_type=F32)


def mm_nt(a, b):
    return lax.dot_general(a, b, (((1,), (1,)), ((), ())), preferred_element_type=F32)


def mm_tn(a, b):
    return lax.dot_general(a, b, (((0,), (0,)), ((), ())), preferred_element_type=F32)


def split(v):
    high = v.astype(BF16)
    return high, (v - high.astype(F32)).astype(BF16)


def kernel(
    nt, nd, width,
    x_hbm, dn_hbm, up_hbm, gain_hbm, head_hbm, lab_hbm, val_hbm,
    out,
    x_ref, dn_ref, up_ref, gain_ref, head_ref, lab_ref, val_ref,
    odn, oup, ogain, stok, rtok, sgram, rgram, pgram, gall, sres, res, sdp, rdp, rin, relay, psum, rcross, sgn, rgn,
    load, sib_s, sib_r, tok_s, tok_r, gr_s, gr_r, ga_s, ga_r, re_s, re_r, fw_s, fw_r, dp_s, dp_r, rel_s, rel_r, cr_s, cr_r,
):
    s, d, t = lax.axis_index("section"), lax.axis_index("dp"), lax.axis_index("tensor")
    first = s == 0
    tokens, feats = x_ref.shape
    rank = dn_ref.shape[1]
    half = tokens // 2
    own = half // nt
    rows = rank // nt
    part = rank // nd
    wire = stok.dtype

    def peer(k, other):
        return (1 - s if other else s, d, lax.rem(t + k, nt))

    group = [(k, o) for k in range(nt) for o in (0, 1) if (k, o) != (0, 0)]

    loads = [
        pltpu.make_async_copy(a, b, load.at[i])
        for i, (a, b) in enumerate((
            (up_hbm, up_ref), (head_hbm, head_ref), (x_hbm, x_ref), (gain_hbm, gain_ref),
            (dn_hbm, dn_ref), (lab_hbm, lab_ref), (val_hbm, val_ref),
        ))
    ]
    for c in loads:
        c.start()

    barrier = pltpu.get_barrier_semaphore()
    for k, o in group:
        pl.semaphore_signal(barrier, inc=1, device_id=peer(k, o), device_id_type=MESH)
    for k in range(1, nd):
        pl.semaphore_signal(barrier, inc=1, device_id=(s, lax.rem(d + k, nd), t), device_id_type=MESH)

    def send(src, dst, ss, rs, to):
        copy = pltpu.make_async_remote_copy(
            src_ref=src, dst_ref=dst, send_sem=ss, recv_sem=rs, device_id=to, device_id_type=MESH
        )
        copy.start()
        return copy

    def put_gram(j, g):
        g = g.astype(wire)
        for i in range(nt):
            sgram[i, j] = g[i * rows : (i + 1) * rows]

    loads[0].wait()
    up = up_ref[...]
    put_gram(0, mm_nt(up, up))
    loads[1].wait()
    head = head_ref[...]
    put_gram(1, mm(up, head))
    for c in loads[2:]:
        c.wait()
    gain = gain_ref[...].astype(F32)
    xb = x_ref[...]
    xf = xb.astype(F32)
    xup = mm_nt(xb, up).astype(wire)
    proj = mm((xf * gain).astype(BF16), dn_ref[...]).astype(wire)
    for b in range(2):
        for i in range(nt):
            at = b * half + i * own
            stok[b, i, 0] = proj[at : at + own]
            stok[b, i, 1] = xup[at : at + own]

    pl.semaphore_wait(barrier, len(group) + nd - 1)

    sib = [
        send(a, b, sib_s.at[i], sib_r.at[i], peer(0, 1))
        for i, (a, b) in enumerate(((up_ref, oup), (dn_ref, odn), (gain_ref, ogain)))
    ]
    started = list(sib)
    spans = (pl.ds(0, 2), pl.ds(2, 1))

    def scatter_gram(j):
        copies = [
            send(
                sgram.at[lax.rem(t + k, nt), spans[j]], rgram.at[k, spans[j]],
                gr_s.at[j, k], gr_r.at[j, k], peer(k, 0),
            )
            for k in range(1, nt)
        ]
        started.extend(copies)
        return copies

    def gather_gram(j, copies):
        total = sgram[t, spans[j]].astype(F32)
        for k in range(1, nt):
            copies[k - 1].wait_recv()
            total = total + rgram[k, spans[j]].astype(F32)
        total = total.astype(wire)
        pgram[spans[j]] = total
        gall[s, t, spans[j]] = total
        out_copies = [
            send(
                pgram.at[spans[j]], gall.at[s, t, spans[j]],
                ga_s.at[j, o, k], ga_r.at[j, o, k], peer(k, o),
            )
            for k, o in group
        ]
        started.extend(out_copies)
        return out_copies

    ab_copies = scatter_gram(0)
    tok_copies = {}
    for k in range(nt):
        to = lax.rem(t + k, nt)
        tok_copies[k, 1] = send(
            stok.at[1 - s, to, pl.ds(0, 2)], rtok.at[1, k, pl.ds(0, 2)],
            tok_s.at[1, k], tok_r.at[1, k], peer(k, 1),
        )
    xm = x_ref[pl.ds(pl.multiple_of(s * half, half), half), :]
    xmf = xm.astype(F32)
    xhead = mm(xm, head)
    squares = jnp.broadcast_to(jnp.sum(xmf * xmf, axis=1, keepdims=True), (half, rank))
    hh, hl = split(xhead)
    qh, ql = split(squares)
    lane_h = lax.broadcasted_iota(jnp.int32, (half, rank), 1)
    q = jnp.where(lane_h < rank // 2, qh.astype(F32), ql.astype(F32)).astype(wire)
    hh, hl = hh.astype(wire), hl.astype(wire)
    for i in range(nt):
        stok[s, i, 2] = hh[i * own : (i + 1) * own]
        stok[s, i, 3] = hl[i * own : (i + 1) * own]
        stok[s, i, 4] = q[i * own : (i + 1) * own]

    sib[0].wait_recv()
    gram_c = mm_nt(up, oup[...])
    gram_d = mm((oup[...].astype(F32) * gain).astype(BF16), dn_ref[...])
    put_gram(2, jnp.where(first, gram_c, gram_d))
    c_copies = scatter_gram(1)
    for k in range(1, nt):
        to = lax.rem(t + k, nt)
        tok_copies[k, 0] = send(
            stok.at[s, to], rtok.at[0, k], tok_s.at[0, k], tok_r.at[0, k], peer(k, 0)
        )
    started += list(tok_copies.values())
    all_copies = gather_gram(0, ab_copies)
    all_copies = all_copies + gather_gram(1, c_copies)

    lab = jnp.where(first, lab_ref[0:1, :], lab_ref[1:2, :])
    val = jnp.where(first, val_ref[0:1, :], val_ref[1:2, :]).astype(F32)
    labels_n = head.shape[1]
    hot_t = jnp.where(lax.broadcasted_iota(jnp.int32, (labels_n, half), 0) == lab, val, 0.0).astype(BF16)
    val_t = jnp.broadcast_to(val, (labels_n, half)).astype(BF16)
    pick = (
        lax.broadcasted_iota(jnp.int32, (own, half), 0) + t * own
        == lax.broadcasted_iota(jnp.int32, (own, half), 1)
    ).astype(F32).astype(BF16)
    onehot = mm_nt(pick, hot_t)
    validity = mm_nt(pick, val_t)
    count = jnp.sum(val_ref[...].astype(F32))

    mine = stok[s, t].astype(F32)
    for k in range(1, nt):
        tok_copies[k, 0].wait_recv()
        mine = mine + rtok[0, k].astype(F32)
    tok_copies[0, 1].wait_recv()
    theirs = rtok[1, 0, 0:2].astype(F32)
    for k in range(1, nt):
        tok_copies[k, 1].wait_recv()
        theirs = theirs + rtok[1, k, 0:2].astype(F32)
    p0 = jnp.where(first, mine[0], theirs[0])
    p1 = jnp.where(first, theirs[0], mine[0])
    v0 = jnp.where(first, mine[1], theirs[1])
    v1 = jnp.where(first, theirs[1], mine[1])
    xh = mine[2] + mine[3]
    sq0 = mine[4][:, 0:1] + mine[4][:, rank // 2 : rank // 2 + 1]

    for c in all_copies:
        c.wait_recv()

    def gram(a, j):
        return gall[a, :, j].reshape(rank, rank).astype(BF16)

    a0, b0, c0 = gram(0, 0), gram(0, 1), gram(0, 2)
    a1, b1, d1 = gram(1, 0), gram(1, 1), gram(1, 2)

    def rowsum(v):
        return jnp.sum(v, axis=1, keepdims=True)

    inv0 = lax.rsqrt(sq0 / width + epsilon)
    pre0 = inv0 * p0
    sig0 = jax.nn.sigmoid(pre0)
    h0 = (pre0 * sig0).astype(BF16)
    h0f = h0.astype(F32)
    h0a = mm(h0, a0)
    p1 = p1 + mm(h0, d1)
    s1u0 = v0 + h0a
    s1u1 = v1 + mm(h0, c0)
    base = xh + mm(h0, b0)
    sq1 = sq0 + rowsum(h0f * (v0 + s1u0))
    inv1 = lax.rsqrt(sq1 / width + epsilon)
    pre1 = inv1 * p1
    sig1 = jax.nn.sigmoid(pre1)
    h1 = (pre1 * sig1).astype(BF16)
    h1f = h1.astype(F32)
    yu1 = s1u1 + mm(h1, a1)
    yu0 = s1u0 + mm_nt(h1, c0)
    base = base + mm(h1, b1)
    sq2 = sq1 + rowsum(h1f * (s1u1 + yu1))
    inv2 = lax.rsqrt(sq2 / width + epsilon)
    logits = inv2 * base
    expo = jnp.exp(logits - jnp.max(logits, axis=1, keepdims=True))
    cot = expo / rowsum(expo) * validity - onehot
    radial = rowsum(cot * base)
    wh = (inv2 * cot).astype(BF16)
    ch = inv2 * inv2 * inv2 / width * radial
    hg1 = mm_nt(wh, b1) - ch * yu1
    act1 = hg1 * sig1 * (1.0 + pre1 * (1.0 - sig1))
    w1 = (inv1 * act1).astype(BF16)
    c1 = inv1 * inv1 * inv1 / width * rowsum(act1 * p1)
    hg0 = mm_nt(wh, b0) - ch * yu0 + mm_nt(w1, d1) - c1 * s1u0
    act0 = hg0 * sig0 * (1.0 + pre0 * (1.0 - sig0))
    w0 = (inv0 * act0).astype(BF16)

    ch_h, ch_l = split(ch)
    c1_h, c1_l = split(c1)
    lane = lax.broadcasted_iota(jnp.int32, (own, rank), 1)
    q4 = rank // 4
    coef = jnp.where(
        lane < q4, ch_h.astype(F32),
        jnp.where(lane < 2 * q4, ch_l.astype(F32), jnp.where(lane < 3 * q4, c1_h.astype(F32), c1_l.astype(F32))),
    )
    for j, v in enumerate((h0, h1, w0, w1, wh, coef)):
        v = v.astype(wire)
        sres[j] = v
        res[s, t, j] = v
    res_copies = {
        k: send(sres, res.at[s, t], re_s.at[k], re_r.at[k], peer(k, 0 if k else 1)) for k in range(nt)
    }
    forwards = []
    for k in range(1, nt):
        res_copies[k].wait_recv()
        at = lax.rem(t + nt - k, nt)
        forwards.append(send(res.at[s, at], res.at[s, at], fw_s.at[k], fw_r.at[k], peer(0, 1)))
    started += list(res_copies.values()) + forwards
    sib[1].wait_recv()
    sib[2].wait_recv()
    res_copies[0].wait_recv()
    for c in forwards:
        c.wait_recv()

    def got(j):
        return res[:, :, j].reshape(tokens, res.shape[-1])

    def piece(j, full):
        full = full.astype(BF16)
        for i in range(nd):
            sdp[i, j] = full[i * part : (i + 1) * part]

    hl = nd // 2
    side = d // hl
    local_d = lax.rem(d, hl)
    far = (1 - side) * hl
    odd = lax.rem(d, 2)
    outer = odd == side

    def remote(src, dst, ss, rs, to):
        return pltpu.make_async_remote_copy(
            src_ref=src, dst_ref=dst, send_sem=ss, recv_sem=rs, device_id=(s, to, t), device_id_type=MESH
        )

    def up_copy(k):
        to = lax.rem(d + k, nd)
        return remote(sdp.at[to, 1], rdp.at[k], dp_s.at[0, k], dp_r.at[0, k], to)

    def near_copy(k):
        to = side * hl + lax.rem(local_d + k, hl)
        return remote(sdp.at[to, 0], rin.at[k], dp_s.at[1, k], dp_r.at[1, k], to)

    def relay_copy():
        return remote(sdp.at[pl.ds(far, hl), 0], relay, rel_s, rel_r, d + 1 - 2 * odd)

    def cross_copy(i):
        m = local_d // 2
        return remote(psum.at[i], rcross.at[m], cr_s.at[i], cr_r.at[m], far + i)

    def cross_wait(m):
        return remote(psum.at[0], rcross.at[m], cr_s.at[0], cr_r.at[m], far)

    def finish(state, own_w, own_h, cotangent):
        scaled = (state * gain).astype(BF16)
        piece(0, mm_tn(own_w, scaled))

        @pl.when(outer)
        def _():
            relay_copy().start()

        gain_row = jnp.sum(mm_nt(own_w, dn_ref[...]) * state, axis=0, keepdims=True)
        sgn[0:1, :] = gain_row
        sgn[1:2, :] = jnp.full((1, feats), count, F32)
        piece(1, mm_tn(own_h, cotangent().astype(BF16)))
        for k in sorted(range(1, nd), key=lambda k: abs(k - hl)):
            up_copy(k).start()
        for k in range(1, hl):
            near_copy(k).start()

    h0g, h1g, w1g, whg = (got(j).astype(BF16) for j in (0, 1, 3, 4))
    cg = got(5).astype(F32)
    chg = cg[:, 0:1] + cg[:, q4 : q4 + 1]
    c1g = cg[:, 2 * q4 : 2 * q4 + 1] + cg[:, 3 * q4 : 3 * q4 + 1]

    @pl.when(s == 0)
    def _():
        def cotangent():
            s1 = xf + mm(h0g, up)
            y = s1 + mm(h1g, oup[...])
            g2 = mm_nt(whg, head) - chg * y
            return g2 + ogain[...].astype(F32) * mm_nt(w1g, odn[...]) - c1g * s1

        finish(xf, got(2).astype(BF16), h0g, cotangent)

    @pl.when(s != 0)
    def _():
        s1 = xf + mm(h0g, oup[...])

        def cotangent():
            y = s1 + mm(h1g, up)
            return mm_nt(whg, head) - chg * y

        finish(s1, w1g, h1g, cotangent)

    small_copies = [
        send(sgn, rgn.at[k], dp_s.at[2, k], dp_r.at[2, k], (s, lax.rem(d + k, nd), t)) for k in range(1, nd)
    ]
    started += small_copies

    @pl.when(jnp.logical_not(outer))
    def _():
        relay_copy().wait_recv()
        psum[...] = (sdp[pl.ds(far, hl), 0].astype(F32) + relay[...].astype(F32)).astype(BF16)
        for i in range(hl):
            cross_copy(i).start()

    small = sgn[...]
    for k in range(1, nd):
        small_copies[k - 1].wait_recv()
        small = small + rgn[k]
    out[2 * part : 2 * part + 2, :] = small
    sums = sdp[d, 1].astype(F32)
    for k in range(1, nd):
        up_copy(k).wait_recv()
        sums = sums + rdp[k].astype(F32)
    out[part : 2 * part, :] = sums
    sums = sdp[d, 0].astype(F32)
    for k in range(1, hl):
        near_copy(k).wait_recv()
        sums = sums + rin[k].astype(F32)
    for m in range(nd // 4):
        cross_wait(m).wait_recv()
        sums = sums + rcross[m].astype(F32)
    out[0:part, :] = sums

    @pl.when(outer)
    def _():
        relay_copy().wait_send()

    @pl.when(jnp.logical_not(outer))
    def _():
        for i in range(hl):
            cross_copy(i).wait_send()

    for k in range(1, nd):
        up_copy(k).wait_send()
    for k in range(1, hl):
        near_copy(k).wait_send()
    for c in started:
        c.wait_send()


def scale_kernel(part, sums, down_out, up_out, gain_out):
    scale = 1.0 / sums[2 * part + 1 : 2 * part + 2, :]
    down_out[...] = sums[0:part, :] * scale
    up_out[...] = sums[part : 2 * part, :] * scale
    gain_out[...] = sums[2 * part : 2 * part + 1, :] * scale


def solution(mesh):
    nt, nd, ns = mesh.shape["tensor"], mesh.shape["dp"], mesh.shape["section"]
    assert ns == 2 and nd % 4 == 0

    def local(inputs, down, up, gains, head, labels, valid):
        micro, per, feats = inputs.shape
        assert micro == ns
        tokens = micro * per
        rank = down.shape[2]
        own, rows, part = tokens // ns // nt, rank // nt, rank // nd
        wire = BF16 if own % 16 == 0 and rows % 16 == 0 else F32
        vmem = pl.BlockSpec(memory_space=pltpu.VMEM)
        dma = pltpu.SemaphoreType.DMA
        anyspace = pl.BlockSpec(memory_space=pl.ANY)
        sums = pl.pallas_call(
            functools.partial(kernel, nt, nd, feats * nt),
            out_shape=jax.ShapeDtypeStruct((2 * part + 8, feats), F32),
            in_specs=[anyspace] * 7,
            out_specs=vmem,
            scratch_shapes=[
                pltpu.VMEM((tokens, feats), BF16),
                pltpu.VMEM((feats, rank), BF16),
                pltpu.VMEM((rank, feats), BF16),
                pltpu.VMEM((1, feats), BF16),
                pltpu.VMEM((feats, head.shape[1]), BF16),
                pltpu.VMEM((micro, per), jnp.int32),
                pltpu.VMEM((micro, per), jnp.int32),
                pltpu.VMEM((feats, rank), BF16),
                pltpu.VMEM((rank, feats), BF16),
                pltpu.VMEM((1, feats), BF16),
                pltpu.VMEM((2, nt, 5, own, rank), wire),
                pltpu.VMEM((2, nt, 5, own, rank), wire),
                pltpu.VMEM((nt, 3, rows, rank), wire),
                pltpu.VMEM((nt, 3, rows, rank), wire),
                pltpu.VMEM((3, rows, rank), wire),
                pltpu.VMEM((2, nt, 3, rows, rank), wire),
                pltpu.VMEM((6, own, rank), wire),
                pltpu.VMEM((2, nt, 6, own, rank), wire),
                pltpu.VMEM((nd, 2, part, feats), BF16),
                pltpu.VMEM((nd, part, feats), BF16),
                pltpu.VMEM((nd // 2, part, feats), BF16),
                pltpu.VMEM((nd // 2, part, feats), BF16),
                pltpu.VMEM((nd // 2, part, feats), BF16),
                pltpu.VMEM((nd // 4, part, feats), BF16),
                pltpu.VMEM((2, feats), F32),
                pltpu.VMEM((nd, 2, feats), F32),
                dma((7,)),
                dma((3,)), dma((3,)),
                dma((2, nt)), dma((2, nt)),
                dma((2, nt)), dma((2, nt)),
                dma((2, 2, nt)), dma((2, 2, nt)),
                dma((nt,)), dma((nt,)),
                dma((nt,)), dma((nt,)),
                dma((3, nd)), dma((3, nd)),
                dma, dma,
                dma((nd // 2,)), dma((nd // 4,)),
            ],
            compiler_params=pltpu.CompilerParams(collective_id=0, has_side_effects=True),
        )(inputs.reshape(tokens, feats), down[0], up[0], gains, head, labels, valid)
        down_t, up_g, gain_g = pl.pallas_call(
            functools.partial(scale_kernel, part),
            out_shape=(
                jax.ShapeDtypeStruct((part, feats), F32),
                jax.ShapeDtypeStruct((part, feats), F32),
                jax.ShapeDtypeStruct((1, feats), F32),
            ),
            in_specs=[vmem],
            out_specs=(vmem,) * 3,
        )(sums)
        return down_t.T[None], up_g[None], gain_g

    return jax.shard_map(
        local,
        mesh=mesh,
        in_specs=(
            P(None, "dp", "tensor"),
            P("section", "tensor", None),
            P("section", None, "tensor"),
            P("section", "tensor"),
            P("tensor", None),
            P(None, "dp"),
            P(None, "dp"),
        ),
        out_specs=(
            P("section", "tensor", "dp"),
            P("section", "dp", "tensor"),
            P("section", "tensor"),
        ),
        check_vma=False,
    )
```
